32 devices in a mesh: rep: 4 (over x, core), mx: 2 (over y), my: 4 (over z).
Axes of the slice: x: 2, y: 2, z: 4, core: 2. Of those that a mesh axis runs over, the one named last changes fastest.
Arguments:
- coefficients: bfloat16 [2, 384, 384, 384], P(None, 'mx', 'my'), may hold values from -7.5 to 7.5
- noise_field: bfloat16 [128, 2, 1536, 1536], P(('rep', 'mx'), None, 'my'), may hold values from -96 to 96
- mode_table: bfloat16 [384, 1536], replicated, may hold values from -0.3125 to 0.3125
Outputs:
- update: bfloat16 [2, 384, 384, 384], P(None, 'mx', 'my', 'rep')
The draws below stay inside these ranges and needn't reach their ends.
All inputs are finite; a program needn't handle non-finite values.
Results may differ from the reference program's by a relative error of at most 0.008.
Values may be sent and summed in bfloat16 or wider, within the bound.
A program may use at most 384 MiB of HBM per device.

```python
import jax
import jax.numpy as jnp
from jax import lax

MODES = 384
POINTS = 1536
PLANES = 128


def steps_of(own_key, extent, pieces, smallest, largest):
    gain, own = 1.0, jax.random.fold_in(own_key, 6)
    for axis_at, shards_of in pieces:
        heights = jnp.exp(jax.random.uniform(jax.random.fold_in(own, axis_at), (shards_of,), jnp.float32, smallest / len(pieces), largest / len(pieces)))
        gain = gain * jnp.repeat(heights, extent[axis_at] // shards_of).reshape([-1 if axis == axis_at else 1 for axis in range(len(extent))])
    return gain


def normal_values(key, dims, scale, bound, cuts=(), dtype=jnp.bfloat16):
    values = scale * jax.random.normal(key, dims, jnp.float32)
    if cuts:
        values = values * steps_of(key, dims, cuts, -0.22, 0.18)
    return jnp.clip(values, -bound, bound).astype(dtype)


def setup_inputs(seed: int = 0) -> dict:
    key_list = jax.random.split(jax.random.key(seed), 4)
    return {
        "coefficients": normal_values(key_list[0], (2, MODES, MODES, MODES), 1.25, 7.5, ((1, 2), (2, 4))),
        "noise_field": normal_values(key_list[1], (PLANES, 2, POINTS, POINTS), 16.0, 96.0, ((0, 8), (2, 4))),
        "mode_table": normal_values(key_list[2], (MODES, POINTS), MODES ** -0.5, 0.3125),
    }


DAMPING = 0.25


def reference(coefficients, noise_field, mode_table):
    slab_first = POINTS // 2 - PLANES // 2
    table_wide = mode_table.astype(jnp.float32)
    slab_table = table_wide[:, slab_first:slab_first + PLANES]
    zmodes = jnp.einsum('pabk,kz->zpab', coefficients.astype(jnp.float32), slab_table).astype(jnp.bfloat16)

    def one_plane(inputs):
        plane_modes, plane_noise = inputs
        xmodes = jnp.einsum('pab,ax->pbx', plane_modes.astype(jnp.float32), table_wide).astype(jnp.bfloat16)
        wave_field = jnp.einsum('pbx,by->pxy', xmodes.astype(jnp.float32), table_wide)
        wave_real = wave_field[0]
        wave_imag = wave_field[1]
        density = wave_real * wave_real + wave_imag * wave_imag
        noise_wide = plane_noise.astype(jnp.float32)
        drive_term = jnp.stack([density * (wave_imag - DAMPING * wave_real) + noise_wide[0],
                                density * (-wave_real - DAMPING * wave_imag) + noise_wide[1]], 0).astype(jnp.bfloat16)
        proj_columns = jnp.einsum('pxy,by->pbx', drive_term.astype(jnp.float32), table_wide).astype(jnp.bfloat16)
        proj_rows = jnp.einsum('pbx,ax->pab', proj_columns.astype(jnp.float32), table_wide).astype(jnp.bfloat16)
        return proj_rows

    projected = lax.map(one_plane, (zmodes, noise_field))
    update = jnp.einsum('zpab,nz->pabn', projected.astype(jnp.float32), slab_table)
    return update.astype(jnp.bfloat16)
```

```python
import jax
import jax.numpy as jnp
from jax import lax
from jax.experimental import pallas as pl
from jax.experimental.pallas import tpu as pltpu
from jax.sharding import PartitionSpec as P

DAMPING = 0.25
MESH = pl.DeviceIdType.MESH
NT = (((1,), (1,)), ((), ()))


def plain_body(coefficients, noise_field, mode_table):
    rep_index = lax.axis_index("rep")
    col_index = lax.axis_index("my")
    rep_count = lax.axis_size("rep")
    row_count = lax.axis_size("mx")
    col_count = lax.axis_size("my")
    planes_dev = noise_field.shape[0]
    planes_rep = planes_dev * row_count
    planes_all = planes_rep * rep_count
    mode_count = mode_table.shape[0]
    point_count = mode_table.shape[1]
    slab_first = point_count // 2 - planes_all // 2
    row_block = mode_count // row_count
    col_block = mode_count // col_count
    point_block = point_count // col_count
    own_block = mode_count // rep_count
    slab_own = lax.dynamic_slice_in_dim(
        mode_table, slab_first + rep_index * planes_rep, planes_rep, 1
    )
    zmodes = jnp.einsum(
        "pabk,kz->zpba", coefficients, slab_own, preferred_element_type=jnp.float32
    ).astype(jnp.bfloat16)
    zmodes = zmodes.reshape(planes_rep, 2, col_block * row_block)
    spread = lax.all_to_all(zmodes, "mx", split_axis=0, concat_axis=2, tiled=True)
    grouped = spread.reshape(planes_dev, 2, row_count, col_block, row_block)
    tiled_table = mode_table.reshape(row_count, row_block, point_count)
    own_points = lax.dynamic_slice_in_dim(tiled_table, col_index * point_block, point_block, 2)
    block_part = jnp.einsum(
        "zpsal,slx->zpax",
        lax.all_gather(grouped, "my", axis=3, tiled=True),
        own_points,
        preferred_element_type=jnp.float32,
    ).astype(jnp.bfloat16)
    wave_field = jnp.einsum(
        "zpax,ay->zpxy", block_part, mode_table, preferred_element_type=jnp.float32
    )
    wave_real = wave_field[:, 0]
    wave_imag = wave_field[:, 1]
    density = wave_real * wave_real + wave_imag * wave_imag
    noise_wide = noise_field.astype(jnp.float32)
    drive_term = jnp.stack(
        [
            density * (wave_imag - DAMPING * wave_real) + noise_wide[:, 0],
            density * (-wave_real - DAMPING * wave_imag) + noise_wide[:, 1],
        ],
        1,
    ).astype(jnp.bfloat16)
    proj_columns = jnp.einsum(
        "zpxy,ny->zpnx", drive_term, mode_table, preferred_element_type=jnp.float32
    ).astype(jnp.bfloat16)
    block_part = lax.all_to_all(proj_columns, "my", split_axis=2, concat_axis=3, tiled=True)
    folded = jnp.einsum(
        "zpax,slx->zpsal", block_part, tiled_table, preferred_element_type=jnp.float32
    ).astype(jnp.bfloat16)
    proj_rows = folded.reshape(
        block_part.shape[0], block_part.shape[1], row_count * col_block * row_block
    )
    gathered_rows = lax.all_to_all(proj_rows, "mx", split_axis=2, concat_axis=0, tiled=True)
    slab_back = lax.dynamic_slice_in_dim(mode_table, rep_index * own_block, own_block, 0)[
        :, slab_first : slab_first + planes_all
    ]
    portion = lax.all_gather(gathered_rows, "rep", axis=0, tiled=True)
    plane_grid = portion.reshape(portion.shape[0], 2, col_block, row_block)
    summed = jnp.einsum("zpba,nz->pabn", plane_grid, slab_back, preferred_element_type=jnp.float32)
    return summed.astype(jnp.bfloat16)

def slab_kernel(own_ref, noise_ref, table_ref, turned_ref, out_ref, modes, parts, landed, noise,
                own_sem, noise_sem, gather_recv, gather_send, sum_recv, sum_send):
    count = lax.axis_size("my")
    me = lax.axis_index("my")
    planes = own_ref.shape[0]
    block = own_ref.shape[2]
    mode_count, point_count = table_ref.shape
    chunk = max(c for c in (512, 256, 128) if point_count % c == 0)
    up = {"my": me + 1}
    down = {"my": me - 1}
    has_up = me < count - 1
    has_down = me > 0

    barrier = pltpu.get_barrier_semaphore()

    @pl.when(has_up)
    def _():
        pl.semaphore_signal(barrier, inc=1, device_id=up, device_id_type=MESH)

    @pl.when(has_down)
    def _():
        pl.semaphore_signal(barrier, inc=1, device_id=down, device_id_type=MESH)

    def rows(j):
        return pl.ds(pl.multiple_of(j * block, block), block)

    def own_copy():
        return pltpu.make_async_copy(own_ref, modes.at[:, :, rows(me)], own_sem)

    def noise_copy(p):
        slot = lax.rem(p, 2)
        return pltpu.make_async_copy(noise_ref.at[p], noise.at[slot], noise_sem.at[slot])

    def gather_copy(p, j, way):
        return pltpu.make_async_remote_copy(
            src_ref=modes.at[p, :, rows(j)],
            dst_ref=modes.at[p, :, rows(j)],
            send_sem=gather_send.at[p, way, j],
            recv_sem=gather_recv.at[p, j],
            device_id=down if way else up,
            device_id_type=MESH,
        )

    def sum_copy(p, j, way, slot):
        return pltpu.make_async_remote_copy(
            src_ref=parts.at[p, :, rows(j)],
            dst_ref=landed.at[p, slot],
            send_sem=sum_send.at[p, way, j],
            recv_sem=sum_recv.at[p, slot],
            device_id=down if way else up,
            device_id_type=MESH,
        )

    own_copy().start()
    noise_copy(0).start()
    if planes > 1:
        noise_copy(1).start()

    pl.semaphore_wait(barrier, has_up.astype(jnp.int32) + has_down.astype(jnp.int32))

    own_copy().wait()

    def inside(p):
        return jnp.logical_and(p >= 0, p < planes)

    def step(s, carry):
        @pl.when(s < planes)
        def _():
            @pl.when(has_up)
            def _():
                gather_copy(s, me, 0).start()

            @pl.when(has_down)
            def _():
                gather_copy(s, me, 1).start()

        for far in range(1, count):
            p = s - far

            @pl.when(jnp.logical_and(inside(p), me - far >= 0))
            def _():
                gather_copy(p, me - far, 0).wait_recv()

                @pl.when(has_up)
                def _():
                    gather_copy(p, me - far, 0).start()

            @pl.when(jnp.logical_and(inside(p), me + far <= count - 1))
            def _():
                gather_copy(p, me + far, 1).wait_recv()

                @pl.when(has_down)
                def _():
                    gather_copy(p, me + far, 1).start()

        c = s - (count - 1)

        @pl.when(inside(c))
        def _():
            noise_copy(c).wait()
            slot = lax.rem(c, 2)
            turned = turned_ref[...]
            lines = [
                lax.dot_general(turned, modes[c, part], NT, preferred_element_type=jnp.float32)
                .astype(jnp.bfloat16)
                for part in range(2)
            ]
            columns = [None, None]
            for first in range(0, point_count, chunk):
                span = slice(first, first + chunk)
                table = table_ref[:, span]
                wave_real, wave_imag = [
                    jnp.dot(line, table, preferred_element_type=jnp.float32) for line in lines
                ]
                density = wave_real * wave_real + wave_imag * wave_imag
                noise_real = noise[slot, 0, :, span].astype(jnp.float32)
                noise_imag = noise[slot, 1, :, span].astype(jnp.float32)
                drive = [
                    density * (wave_imag - DAMPING * wave_real) + noise_real,
                    density * (-wave_real - DAMPING * wave_imag) + noise_imag,
                ]
                for part in range(2):
                    more = lax.dot_general(
                        table, drive[part].astype(jnp.bfloat16), NT,
                        preferred_element_type=jnp.float32,
                    )
                    columns[part] = more if first == 0 else columns[part] + more
            for part in range(2):
                parts[c, part] = jnp.dot(
                    columns[part].astype(jnp.bfloat16), turned, preferred_element_type=jnp.float32
                ).astype(jnp.bfloat16)

            @pl.when(c + 2 < planes)
            def _():
                noise_copy(c + 2).start()

        def add(p, j, slot):
            wide = parts[p, :, rows(j)].astype(jnp.float32) + landed[p, slot].astype(jnp.float32)
            parts[p, :, rows(j)] = wide.astype(jnp.bfloat16)

        rising = c - me
        for far in range(count - 1, 0, -1):
            @pl.when(jnp.logical_and(inside(rising), me + far <= count - 1))
            def _():
                j = me + far

                @pl.when(has_down)
                def _():
                    sum_copy(rising, j, 0, j).wait_recv()
                    add(rising, j, j)

                sum_copy(rising, j, 0, j).start()

        sinking = c - (count - 1 - me)
        for far in range(count - 1, 0, -1):
            @pl.when(jnp.logical_and(inside(sinking), me - far >= 0))
            def _():
                j = me - far

                @pl.when(has_up)
                def _():
                    sum_copy(sinking, j, 1, j).wait_recv()
                    add(sinking, j, j)

                sum_copy(sinking, j, 1, count if far == 1 else j).start()

        done = c - count

        @pl.when(inside(done))
        def _():
            @pl.when(has_down)
            def _():
                sum_copy(done, me, 0, me).wait_recv()
                add(done, me, me)

            @pl.when(has_up)
            def _():
                sum_copy(done, me, 1, count).wait_recv()
                add(done, me, count)

            out_ref[done] = parts[done, :, rows(me)]

        return carry

    lax.fori_loop(0, planes + 2 * count - 1, step, 0)

    def finish(p, carry):
        for j in range(count):
            @pl.when(jnp.logical_and(has_up, j <= me))
            def _():
                gather_copy(p, j, 0).wait_send()

            @pl.when(jnp.logical_and(has_down, j >= me))
            def _():
                gather_copy(p, j, 1).wait_send()

            @pl.when(j > me)
            def _():
                sum_copy(p, j, 0, j).wait_send()

            @pl.when(j < me)
            def _():
                sum_copy(p, j, 1, j).wait_send()

        return carry

    lax.fori_loop(0, planes, finish, 0)


def slab_planes(own_modes, noise_field, mode_table, turned):
    count = lax.axis_size("my")
    planes, _, block, mode_count = own_modes.shape
    point_block, point_count = noise_field.shape[2:]
    vmem = pl.BlockSpec(memory_space=pltpu.VMEM)
    hbm = pl.BlockSpec(memory_space=pl.ANY)
    dma = pltpu.SemaphoreType.DMA
    flops = 8 * planes * mode_count * point_block * (point_count + mode_count)
    return pl.pallas_call(
        slab_kernel,
        out_shape=jax.ShapeDtypeStruct(own_modes.shape, jnp.bfloat16),
        in_specs=[hbm, hbm, vmem, vmem],
        out_specs=vmem,
        scratch_shapes=[
            pltpu.VMEM((planes, 2, mode_count, mode_count), jnp.bfloat16),
            pltpu.VMEM((planes, 2, mode_count, mode_count), jnp.bfloat16),
            pltpu.VMEM((planes, count + 1, 2, block, mode_count), jnp.bfloat16),
            pltpu.VMEM((2, 2, point_block, point_count), jnp.bfloat16),
            dma,
            dma((2,)),
            dma((planes, count)),
            dma((planes, 2, count)),
            dma((planes, count + 1)),
            dma((planes, 2, count)),
        ],
        compiler_params=pltpu.CompilerParams(
            collective_id=0, has_side_effects=True, vmem_limit_bytes=60 * 1024 * 1024
        ),
        cost_estimate=pl.CostEstimate(
            flops=flops, bytes_accessed=noise_field.size * 2, transcendentals=0
        ),
    )(own_modes, noise_field, mode_table, turned)


def body(coefficients, noise_field, mode_table):
    rep_index = lax.axis_index("rep")
    col_index = lax.axis_index("my")
    rep_count = lax.axis_size("rep")
    row_count = lax.axis_size("mx")
    col_count = lax.axis_size("my")
    planes_dev = noise_field.shape[0]
    planes_rep = planes_dev * row_count
    planes_all = planes_rep * rep_count
    mode_count = mode_table.shape[0]
    point_count = mode_table.shape[1]
    slab_first = point_count // 2 - planes_all // 2
    row_block = mode_count // row_count
    col_block = mode_count // col_count
    point_block = point_count // col_count
    own_block = mode_count // rep_count
    if col_block % 16 or point_block % 128 or mode_count % 128 or col_count < 2:
        return plain_body(coefficients, noise_field, mode_table)
    slab_own = lax.dynamic_slice_in_dim(
        mode_table, slab_first + rep_index * planes_rep, planes_rep, 1
    )
    zmodes = jnp.einsum(
        "pabk,kz->zpba", coefficients, slab_own, preferred_element_type=jnp.float32
    ).astype(jnp.bfloat16)
    zmodes = zmodes.reshape(planes_rep, 2, col_block * row_block)
    spread = lax.all_to_all(zmodes, "mx", split_axis=0, concat_axis=2, tiled=True)
    own_modes = (
        spread.reshape(planes_dev, 2, row_count, col_block, row_block)
        .transpose(0, 1, 3, 2, 4)
        .reshape(planes_dev, 2, col_block, mode_count)
    )
    turned = lax.dynamic_slice_in_dim(mode_table, col_index * point_block, point_block, 1).T
    proj_rows = slab_planes(own_modes, noise_field, mode_table, turned)
    gathered_rows = lax.all_to_all(proj_rows, "mx", split_axis=3, concat_axis=0, tiled=True)
    slab_back = lax.dynamic_slice_in_dim(mode_table, rep_index * own_block, own_block, 0)[
        :, slab_first : slab_first + planes_all
    ]
    portion = lax.all_gather(
        gathered_rows.reshape(planes_rep, 2, col_block * row_block), "rep", axis=0, tiled=True
    )
    plane_grid = portion.reshape(planes_all, 2, col_block, row_block)
    summed = jnp.einsum("zpba,nz->pabn", plane_grid, slab_back, preferred_element_type=jnp.float32)
    return summed.astype(jnp.bfloat16)


def solution(mesh):
    in_specs = (P(None, "mx", "my", None), P(("rep", "mx"), None, "my", None), P())
    out_specs = P(None, "mx", "my", "rep")
    return jax.shard_map(body, mesh=mesh, in_specs=in_specs, out_specs=out_specs, check_vma=False)
```

```python
import jax
import jax.numpy as jnp
from jax import lax
from jax.experimental import pallas as pl
from jax.experimental.pallas import tpu as pltpu
from jax.sharding import PartitionSpec as P

DAMPING = 0.25
MESH = pl.DeviceIdType.MESH
NT = (((1,), (1,)), ((), ()))


def plain_body(coefficients, noise_field, mode_table):
    rep_index = lax.axis_index("rep")
    col_index = lax.axis_index("my")
    rep_count = lax.axis_size("rep")
    row_count = lax.axis_size("mx")
    col_count = lax.axis_size("my")
    planes_dev = noise_field.shape[0]
    planes_rep = planes_dev * row_count
    planes_all = planes_rep * rep_count
    mode_count = mode_table.shape[0]
    point_count = mode_table.shape[1]
    slab_first = point_count // 2 - planes_all // 2
    row_block = mode_count // row_count
    col_block = mode_count // col_count
    point_block = point_count // col_count
    own_block = mode_count // rep_count
    slab_own = lax.dynamic_slice_in_dim(
        mode_table, slab_first + rep_index * planes_rep, planes_rep, 1
    )
    zmodes = jnp.einsum(
        "pabk,kz->zpba", coefficients, slab_own, preferred_element_type=jnp.float32
    ).astype(jnp.bfloat16)
    zmodes = zmodes.reshape(planes_rep, 2, col_block * row_block)
    spread = lax.all_to_all(zmodes, "mx", split_axis=0, concat_axis=2, tiled=True)
    grouped = spread.reshape(planes_dev, 2, row_count, col_block, row_block)
    tiled_table = mode_table.reshape(row_count, row_block, point_count)
    own_points = lax.dynamic_slice_in_dim(tiled_table, col_index * point_block, point_block, 2)
    block_part = jnp.einsum(
        "zpsal,slx->zpax",
        lax.all_gather(grouped, "my", axis=3, tiled=True),
        own_points,
        preferred_element_type=jnp.float32,
    ).astype(jnp.bfloat16)
    wave_field = jnp.einsum(
        "zpax,ay->zpxy", block_part, mode_table, preferred_element_type=jnp.float32
    )
    wave_real = wave_field[:, 0]
    wave_imag = wave_field[:, 1]
    density = wave_real * wave_real + wave_imag * wave_imag
    noise_wide = noise_field.astype(jnp.float32)
    drive_term = jnp.stack(
        [
            density * (wave_imag - DAMPING * wave_real) + noise_wide[:, 0],
            density * (-wave_real - DAMPING * wave_imag) + noise_wide[:, 1],
        ],
        1,
    ).astype(jnp.bfloat16)
    proj_columns = jnp.einsum(
        "zpxy,ny->zpnx", drive_term, mode_table, preferred_element_type=jnp.float32
    ).astype(jnp.bfloat16)
    block_part = lax.all_to_all(proj_columns, "my", split_axis=2, concat_axis=3, tiled=True)
    folded = jnp.einsum(
        "zpax,slx->zpsal", block_part, tiled_table, preferred_element_type=jnp.float32
    ).astype(jnp.bfloat16)
    proj_rows = folded.reshape(
        block_part.shape[0], block_part.shape[1], row_count * col_block * row_block
    )
    gathered_rows = lax.all_to_all(proj_rows, "mx", split_axis=2, concat_axis=0, tiled=True)
    slab_back = lax.dynamic_slice_in_dim(mode_table, rep_index * own_block, own_block, 0)[
        :, slab_first : slab_first + planes_all
    ]
    portion = lax.all_gather(gathered_rows, "rep", axis=0, tiled=True)
    plane_grid = portion.reshape(portion.shape[0], 2, col_block, row_block)
    summed = jnp.einsum("zpba,nz->pabn", plane_grid, slab_back, preferred_element_type=jnp.float32)
    return summed.astype(jnp.bfloat16)

def slab_kernel(own_ref, noise_ref, table_ref, turned_ref, out_ref, modes, parts, landed, noise,
                halves, own_sem, noise_sem, gather_recv, gather_send, sum_recv, sum_send,
                half_recv, half_send, last_recv, last_send):
    count = lax.axis_size("my")
    me = lax.axis_index("my")
    row_count = lax.axis_size("mx")
    row = lax.axis_index("mx")
    rep_count = lax.axis_size("rep")
    rep = lax.axis_index("rep")
    planes = own_ref.shape[0] // row_count
    block = own_ref.shape[2]
    row_block = own_ref.shape[3]
    offsets = [(dr, dh) for dr in range(rep_count) for dh in range(row_count)]
    mode_count, point_count = table_ref.shape
    chunk = max(c for c in (512, 256, 128) if point_count % c == 0)
    up = {"my": me + 1}
    down = {"my": me - 1}
    has_up = me < count - 1
    has_down = me > 0

    barrier = pltpu.get_barrier_semaphore()

    @pl.when(has_up)
    def _():
        pl.semaphore_signal(barrier, inc=1, device_id=up, device_id_type=MESH)

    @pl.when(has_down)
    def _():
        pl.semaphore_signal(barrier, inc=1, device_id=down, device_id_type=MESH)

    for dr, dh in offsets[1:]:
        pl.semaphore_signal(
            barrier, inc=1,
            device_id={"rep": lax.rem(rep + dr, rep_count), "mx": lax.rem(row + dh, row_count)},
            device_id_type=MESH,
        )

    def rows(j):
        return pl.ds(pl.multiple_of(j * block, block), block)

    def own_copy():
        return pltpu.make_async_copy(
            own_ref.at[pl.ds(row * planes, planes)], halves.at[:, row], own_sem
        )

    def half_copy(p, dh, source):
        target = lax.rem(row + dh, row_count)
        return pltpu.make_async_remote_copy(
            src_ref=own_ref.at[target * planes + p],
            dst_ref=halves.at[p, source],
            send_sem=half_send.at[p, dh],
            recv_sem=half_recv.at[p, dh],
            device_id={"mx": target},
            device_id_type=MESH,
        )

    def last_copy(p, at, received):
        dr, dh = offsets[at]
        target = lax.rem(row + dh, row_count)
        if received:
            from_rep = lax.rem(rep + rep_count - dr, rep_count)
            from_row = lax.rem(row + row_count - dh, row_count)
        else:
            from_rep, from_row = rep, row
        plane = (from_rep * row_count + from_row) * planes + p
        if at == 0:
            return pltpu.make_async_copy(halves.at[p, row], out_ref.at[plane], last_send.at[p, 0])
        return pltpu.make_async_remote_copy(
            src_ref=halves.at[p, target],
            dst_ref=out_ref.at[plane],
            send_sem=last_send.at[p, at],
            recv_sem=last_recv.at[p, at],
            device_id={"rep": lax.rem(rep + dr, rep_count), "mx": target},
            device_id_type=MESH,
        )

    def noise_copy(p):
        slot = lax.rem(p, 2)
        return pltpu.make_async_copy(noise_ref.at[p], noise.at[slot], noise_sem.at[slot])

    def gather_copy(p, j, way):
        return pltpu.make_async_remote_copy(
            src_ref=modes.at[p, :, rows(j)],
            dst_ref=modes.at[p, :, rows(j)],
            send_sem=gather_send.at[p, way, j],
            recv_sem=gather_recv.at[p, j],
            device_id=down if way else up,
            device_id_type=MESH,
        )

    def sum_copy(p, j, way, slot):
        return pltpu.make_async_remote_copy(
            src_ref=parts.at[p, :, rows(j)],
            dst_ref=landed.at[p, slot],
            send_sem=sum_send.at[p, way, j],
            recv_sem=sum_recv.at[p, slot],
            device_id=down if way else up,
            device_id_type=MESH,
        )

    own_copy().start()
    noise_copy(0).start()
    if planes > 1:
        noise_copy(1).start()

    pl.semaphore_wait(barrier, has_up.astype(jnp.int32) + has_down.astype(jnp.int32) + len(offsets) - 1)

    def send_half(p, carry):
        for dh in range(1, row_count):
            half_copy(p, dh, row).start()
        return carry

    lax.fori_loop(0, planes, send_half, 0)
    own_copy().wait()

    def inside(p):
        return jnp.logical_and(p >= 0, p < planes)

    def step(s, carry):
        @pl.when(s < planes)
        def _():
            for dh in range(1, row_count):
                half_copy(s, dh, lax.rem(row + row_count - dh, row_count)).wait_recv()
            for part in range(2):
                modes[s, part, rows(me)] = jnp.concatenate(
                    [halves[s, h, part] for h in range(row_count)], 1
                )

            @pl.when(has_up)
            def _():
                gather_copy(s, me, 0).start()

            @pl.when(has_down)
            def _():
                gather_copy(s, me, 1).start()

        for far in range(1, count):
            p = s - far

            @pl.when(jnp.logical_and(inside(p), me - far >= 0))
            def _():
                gather_copy(p, me - far, 0).wait_recv()

                @pl.when(has_up)
                def _():
                    gather_copy(p, me - far, 0).start()

            @pl.when(jnp.logical_and(inside(p), me + far <= count - 1))
            def _():
                gather_copy(p, me + far, 1).wait_recv()

                @pl.when(has_down)
                def _():
                    gather_copy(p, me + far, 1).start()

        c = s - (count - 1)

        @pl.when(inside(c))
        def _():
            noise_copy(c).wait()
            slot = lax.rem(c, 2)
            turned = turned_ref[...]
            lines = [
                lax.dot_general(turned, modes[c, part], NT, preferred_element_type=jnp.float32)
                .astype(jnp.bfloat16)
                for part in range(2)
            ]
            columns = [None, None]
            for first in range(0, point_count, chunk):
                span = slice(first, first + chunk)
                table = table_ref[:, span]
                wave_real, wave_imag = [
                    jnp.dot(line, table, preferred_element_type=jnp.float32) for line in lines
                ]
                density = wave_real * wave_real + wave_imag * wave_imag
                noise_real = noise[slot, 0, :, span].astype(jnp.float32)
                noise_imag = noise[slot, 1, :, span].astype(jnp.float32)
                drive = [
                    density * (wave_imag - DAMPING * wave_real) + noise_real,
                    density * (-wave_real - DAMPING * wave_imag) + noise_imag,
                ]
                for part in range(2):
                    more = lax.dot_general(
                        table, drive[part].astype(jnp.bfloat16), NT,
                        preferred_element_type=jnp.float32,
                    )
                    columns[part] = more if first == 0 else columns[part] + more
            for part in range(2):
                parts[c, part] = jnp.dot(
                    columns[part].astype(jnp.bfloat16), turned, preferred_element_type=jnp.float32
                ).astype(jnp.bfloat16)

            @pl.when(c + 2 < planes)
            def _():
                noise_copy(c + 2).start()

        def add(p, j, slot):
            wide = parts[p, :, rows(j)].astype(jnp.float32) + landed[p, slot].astype(jnp.float32)
            parts[p, :, rows(j)] = wide.astype(jnp.bfloat16)

        rising = c - me
        for far in range(count - 1, 0, -1):
            @pl.when(jnp.logical_and(inside(rising), me + far <= count - 1))
            def _():
                j = me + far

                @pl.when(has_down)
                def _():
                    sum_copy(rising, j, 0, j).wait_recv()
                    add(rising, j, j)

                sum_copy(rising, j, 0, j).start()

        sinking = c - (count - 1 - me)
        for far in range(count - 1, 0, -1):
            @pl.when(jnp.logical_and(inside(sinking), me - far >= 0))
            def _():
                j = me - far

                @pl.when(has_up)
                def _():
                    sum_copy(sinking, j, 1, j).wait_recv()
                    add(sinking, j, j)

                sum_copy(sinking, j, 1, count if far == 1 else j).start()

        done = c - count

        @pl.when(inside(done))
        def _():
            @pl.when(has_down)
            def _():
                sum_copy(done, me, 0, me).wait_recv()
                add(done, me, me)

            @pl.when(has_up)
            def _():
                sum_copy(done, me, 1, count).wait_recv()
                add(done, me, count)

            for part in range(2):
                whole = parts[done, part, rows(me)]
                for h in range(row_count):
                    halves[done, h, part] = whole[:, h * row_block : (h + 1) * row_block]
            for at in range(len(offsets)):
                last_copy(done, at, False).start()

        return carry

    lax.fori_loop(0, planes + 2 * count - 1, step, 0)

    def finish(p, carry):
        for j in range(count):
            @pl.when(jnp.logical_and(has_up, j <= me))
            def _():
                gather_copy(p, j, 0).wait_send()

            @pl.when(jnp.logical_and(has_down, j >= me))
            def _():
                gather_copy(p, j, 1).wait_send()

            @pl.when(j > me)
            def _():
                sum_copy(p, j, 0, j).wait_send()

            @pl.when(j < me)
            def _():
                sum_copy(p, j, 1, j).wait_send()

        for dh in range(1, row_count):
            half_copy(p, dh, row).wait_send()
        last_copy(p, 0, False).wait()
        for at in range(1, len(offsets)):
            last_copy(p, at, False).wait_send()
            last_copy(p, at, True).wait_recv()
        return carry

    lax.fori_loop(0, planes, finish, 0)


def slab_planes(own_modes, noise_field, mode_table, turned):
    count = lax.axis_size("my")
    mode_count = mode_table.shape[0]
    row_count = lax.axis_size("mx")
    rep_count = lax.axis_size("rep")
    planes_rep, _, block, row_block = own_modes.shape
    planes = planes_rep // row_count
    point_block, point_count = noise_field.shape[2:]
    vmem = pl.BlockSpec(memory_space=pltpu.VMEM)
    hbm = pl.BlockSpec(memory_space=pl.ANY)
    dma = pltpu.SemaphoreType.DMA
    flops = 8 * planes * mode_count * point_block * (point_count + mode_count)
    return pl.pallas_call(
        slab_kernel,
        out_shape=jax.ShapeDtypeStruct((planes_rep * rep_count, 2, block, row_block), jnp.bfloat16),
        in_specs=[hbm, hbm, vmem, vmem],
        out_specs=hbm,
        scratch_shapes=[
            pltpu.VMEM((planes, 2, mode_count, mode_count), jnp.bfloat16),
            pltpu.VMEM((planes, 2, mode_count, mode_count), jnp.bfloat16),
            pltpu.VMEM((planes, count + 1, 2, block, mode_count), jnp.bfloat16),
            pltpu.VMEM((2, 2, point_block, point_count), jnp.bfloat16),
            pltpu.VMEM((planes, row_count, 2, block, row_block), jnp.bfloat16),
            dma,
            dma((2,)),
            dma((planes, count)),
            dma((planes, 2, count)),
            dma((planes, count + 1)),
            dma((planes, 2, count)),
            dma((planes, row_count)),
            dma((planes, row_count)),
            dma((planes, row_count * rep_count)),
            dma((planes, row_count * rep_count)),
        ],
        compiler_params=pltpu.CompilerParams(
            collective_id=0, has_side_effects=True, vmem_limit_bytes=60 * 1024 * 1024
        ),
        cost_estimate=pl.CostEstimate(
            flops=flops, bytes_accessed=noise_field.size * 2, transcendentals=0
        ),
    )(own_modes, noise_field, mode_table, turned)


def body(coefficients, noise_field, mode_table):
    rep_index = lax.axis_index("rep")
    col_index = lax.axis_index("my")
    rep_count = lax.axis_size("rep")
    row_count = lax.axis_size("mx")
    col_count = lax.axis_size("my")
    planes_dev = noise_field.shape[0]
    planes_rep = planes_dev * row_count
    planes_all = planes_rep * rep_count
    mode_count = mode_table.shape[0]
    point_count = mode_table.shape[1]
    slab_first = point_count // 2 - planes_all // 2
    row_block = mode_count // row_count
    col_block = mode_count // col_count
    point_block = point_count // col_count
    own_block = mode_count // rep_count
    if col_block % 16 or point_block % 128 or mode_count % 128 or col_count < 2:
        return plain_body(coefficients, noise_field, mode_table)
    slab_own = lax.dynamic_slice_in_dim(
        mode_table, slab_first + rep_index * planes_rep, planes_rep, 1
    )
    zmodes = jnp.einsum(
        "pabk,kz->zpba", coefficients, slab_own, preferred_element_type=jnp.float32
    ).astype(jnp.bfloat16)
    turned = lax.dynamic_slice_in_dim(mode_table, col_index * point_block, point_block, 1).T
    plane_grid = slab_planes(zmodes, noise_field, mode_table, turned)
    slab_back = lax.dynamic_slice_in_dim(mode_table, rep_index * own_block, own_block, 0)[
        :, slab_first : slab_first + planes_all
    ]
    summed = jnp.einsum("zpba,nz->pabn", plane_grid, slab_back, preferred_element_type=jnp.float32)
    return summed.astype(jnp.bfloat16)


def solution(mesh):
    in_specs = (P(None, "mx", "my", None), P(("rep", "mx"), None, "my", None), P())
    out_specs = P(None, "mx", "my", "rep")
    return jax.shard_map(body, mesh=mesh, in_specs=in_specs, out_specs=out_specs, check_vma=False)
```

```python
import jax
import jax.numpy as jnp
from jax import lax
from jax.experimental import pallas as pl
from jax.experimental.pallas import tpu as pltpu
from jax.sharding import PartitionSpec as P

DAMPING = 0.25
MESH = pl.DeviceIdType.MESH
NT = (((1,), (1,)), ((), ()))


def plain_body(coefficients, noise_field, mode_table):
    rep_index = lax.axis_index("rep")
    col_index = lax.axis_index("my")
    rep_count = lax.axis_size("rep")
    row_count = lax.axis_size("mx")
    col_count = lax.axis_size("my")
    planes_dev = noise_field.shape[0]
    planes_rep = planes_dev * row_count
    planes_all = planes_rep * rep_count
    mode_count = mode_table.shape[0]
    point_count = mode_table.shape[1]
    slab_first = point_count // 2 - planes_all // 2
    row_block = mode_count // row_count
    col_block = mode_count // col_count
    point_block = point_count // col_count
    own_block = mode_count // rep_count
    slab_own = lax.dynamic_slice_in_dim(
        mode_table, slab_first + rep_index * planes_rep, planes_rep, 1
    )
    zmodes = jnp.einsum(
        "pabk,kz->zpba", coefficients, slab_own, preferred_element_type=jnp.float32
    ).astype(jnp.bfloat16)
    zmodes = zmodes.reshape(planes_rep, 2, col_block * row_block)
    spread = lax.all_to_all(zmodes, "mx", split_axis=0, concat_axis=2, tiled=True)
    grouped = spread.reshape(planes_dev, 2, row_count, col_block, row_block)
    tiled_table = mode_table.reshape(row_count, row_block, point_count)
    own_points = lax.dynamic_slice_in_dim(tiled_table, col_index * point_block, point_block, 2)
    block_part = jnp.einsum(
        "zpsal,slx->zpax",
        lax.all_gather(grouped, "my", axis=3, tiled=True),
        own_points,
        preferred_element_type=jnp.float32,
    ).astype(jnp.bfloat16)
    wave_field = jnp.einsum(
        "zpax,ay->zpxy", block_part, mode_table, preferred_element_type=jnp.float32
    )
    wave_real = wave_field[:, 0]
    wave_imag = wave_field[:, 1]
    density = wave_real * wave_real + wave_imag * wave_imag
    noise_wide = noise_field.astype(jnp.float32)
    drive_term = jnp.stack(
        [
            density * (wave_imag - DAMPING * wave_real) + noise_wide[:, 0],
            density * (-wave_real - DAMPING * wave_imag) + noise_wide[:, 1],
        ],
        1,
    ).astype(jnp.bfloat16)
    proj_columns = jnp.einsum(
        "zpxy,ny->zpnx", drive_term, mode_table, preferred_element_type=jnp.float32
    ).astype(jnp.bfloat16)
    block_part = lax.all_to_all(proj_columns, "my", split_axis=2, concat_axis=3, tiled=True)
    folded = jnp.einsum(
        "zpax,slx->zpsal", block_part, tiled_table, preferred_element_type=jnp.float32
    ).astype(jnp.bfloat16)
    proj_rows = folded.reshape(
        block_part.shape[0], block_part.shape[1], row_count * col_block * row_block
    )
    gathered_rows = lax.all_to_all(proj_rows, "mx", split_axis=2, concat_axis=0, tiled=True)
    slab_back = lax.dynamic_slice_in_dim(mode_table, rep_index * own_block, own_block, 0)[
        :, slab_first : slab_first + planes_all
    ]
    portion = lax.all_gather(gathered_rows, "rep", axis=0, tiled=True)
    plane_grid = portion.reshape(portion.shape[0], 2, col_block, row_block)
    summed = jnp.einsum("zpba,nz->pabn", plane_grid, slab_back, preferred_element_type=jnp.float32)
    return summed.astype(jnp.bfloat16)

def slab_kernel(own_ref, noise_ref, table_ref, turned_ref, out_ref, modes, parts, landed, noise,
                halves, own_sem, noise_sem, gather_recv, gather_send, sum_recv, sum_send,
                half_recv, half_send, last_recv, last_send):
    count = lax.axis_size("my")
    me = lax.axis_index("my")
    row_count = lax.axis_size("mx")
    row = lax.axis_index("mx")
    rep_count = lax.axis_size("rep")
    rep = lax.axis_index("rep")
    planes = own_ref.shape[0] // row_count
    block = own_ref.shape[2]
    row_block = own_ref.shape[3]
    offsets = [(dr, dh) for dr in range(rep_count) for dh in range(row_count)]
    mode_count, point_count = table_ref.shape
    chunk = max(c for c in (512, 256, 128) if point_count % c == 0)
    up = {"my": me + 1}
    down = {"my": me - 1}
    has_up = me < count - 1
    has_down = me > 0

    barrier = pltpu.get_barrier_semaphore()

    @pl.when(has_up)
    def _():
        pl.semaphore_signal(barrier, inc=1, device_id=up, device_id_type=MESH)

    @pl.when(has_down)
    def _():
        pl.semaphore_signal(barrier, inc=1, device_id=down, device_id_type=MESH)

    for dr, dh in offsets[1:]:
        pl.semaphore_signal(
            barrier, inc=1,
            device_id={"rep": lax.rem(rep + dr, rep_count), "mx": lax.rem(row + dh, row_count)},
            device_id_type=MESH,
        )

    def rows(j):
        return pl.ds(pl.multiple_of(j * block, block), block)

    def own_copy():
        return pltpu.make_async_copy(
            own_ref.at[pl.ds(row * planes, planes)], halves.at[:, row], own_sem
        )

    def half_copy(p, dh, source):
        target = lax.rem(row + dh, row_count)
        return pltpu.make_async_remote_copy(
            src_ref=own_ref.at[target * planes + p],
            dst_ref=halves.at[p, source],
            send_sem=half_send.at[p, dh],
            recv_sem=half_recv.at[p, dh],
            device_id={"mx": target},
            device_id_type=MESH,
        )

    def last_copy(p, at, received):
        dr, dh = offsets[at]
        target = lax.rem(row + dh, row_count)
        if received:
            from_rep = lax.rem(rep + rep_count - dr, rep_count)
            from_row = lax.rem(row + row_count - dh, row_count)
        else:
            from_rep, from_row = rep, row
        plane = (from_rep * row_count + from_row) * planes + p
        if at == 0:
            return pltpu.make_async_copy(halves.at[p, row], out_ref.at[plane], last_send.at[p, 0])
        return pltpu.make_async_remote_copy(
            src_ref=halves.at[p, target],
            dst_ref=out_ref.at[plane],
            send_sem=last_send.at[p, at],
            recv_sem=last_recv.at[p, at],
            device_id={"rep": lax.rem(rep + dr, rep_count), "mx": target},
            device_id_type=MESH,
        )

    def noise_copy(p):
        slot = lax.rem(p, 2)
        return pltpu.make_async_copy(noise_ref.at[p], noise.at[slot], noise_sem.at[slot])

    def gather_copy(p, j, way):
        return pltpu.make_async_remote_copy(
            src_ref=modes.at[p, :, rows(j)],
            dst_ref=modes.at[p, :, rows(j)],
            send_sem=gather_send.at[p, way, j],
            recv_sem=gather_recv.at[p, j],
            device_id=down if way else up,
            device_id_type=MESH,
        )

    def sum_copy(p, j, way, slot):
        return pltpu.make_async_remote_copy(
            src_ref=parts.at[p, :, rows(j)],
            dst_ref=landed.at[p, slot],
            send_sem=sum_send.at[p, way, j],
            recv_sem=sum_recv.at[p, slot],
            device_id=down if way else up,
            device_id_type=MESH,
        )

    own_copy().start()
    noise_copy(0).start()
    if planes > 1:
        noise_copy(1).start()

    pl.semaphore_wait(barrier, has_up.astype(jnp.int32) + has_down.astype(jnp.int32) + len(offsets) - 1)

    def send_half(p, carry):
        for dh in range(1, row_count):
            half_copy(p, dh, row).start()
        return carry

    lax.fori_loop(0, planes, send_half, 0)
    own_copy().wait()

    def inside(p):
        return jnp.logical_and(p >= 0, p < planes)

    def step(s, carry):
        @pl.when(s < planes)
        def _():
            for dh in range(1, row_count):
                half_copy(s, dh, lax.rem(row + row_count - dh, row_count)).wait_recv()
            for part in range(2):
                modes[s, part, rows(me)] = jnp.concatenate(
                    [halves[s, h, part] for h in range(row_count)], 1
                )

            @pl.when(has_up)
            def _():
                gather_copy(s, me, 0).start()

            @pl.when(has_down)
            def _():
                gather_copy(s, me, 1).start()

        for far in range(1, count):
            p = s - far

            @pl.when(jnp.logical_and(inside(p), me - far >= 0))
            def _():
                gather_copy(p, me - far, 0).wait_recv()

                @pl.when(has_up)
                def _():
                    gather_copy(p, me - far, 0).start()

            @pl.when(jnp.logical_and(inside(p), me + far <= count - 1))
            def _():
                gather_copy(p, me + far, 1).wait_recv()

                @pl.when(has_down)
                def _():
                    gather_copy(p, me + far, 1).start()

        c = s - (count - 1)

        @pl.when(inside(c))
        def _():
            noise_copy(c).wait()
            slot = lax.rem(c, 2)
            turned = turned_ref[...]
            lines = [
                lax.dot_general(turned, modes[c, part], NT, preferred_element_type=jnp.float32)
                .astype(jnp.bfloat16)
                for part in range(2)
            ]
            columns = [None, None]
            for first in range(0, point_count, chunk):
                span = slice(first, first + chunk)
                table = table_ref[:, span]
                wave_real, wave_imag = [
                    jnp.dot(line, table, preferred_element_type=jnp.float32) for line in lines
                ]
                density = wave_real * wave_real + wave_imag * wave_imag
                noise_real = noise[slot, 0, :, span].astype(jnp.float32)
                noise_imag = noise[slot, 1, :, span].astype(jnp.float32)
                drive = [
                    density * (wave_imag - DAMPING * wave_real) + noise_real,
                    density * (-wave_real - DAMPING * wave_imag) + noise_imag,
                ]
                for part in range(2):
                    more = lax.dot_general(
                        table, drive[part].astype(jnp.bfloat16), NT,
                        preferred_element_type=jnp.float32,
                    )
                    columns[part] = more if first == 0 else columns[part] + more
            for part in range(2):
                parts[c, part] = jnp.dot(
                    columns[part].astype(jnp.bfloat16), turned, preferred_element_type=jnp.float32
                ).astype(jnp.bfloat16)

            @pl.when(c + 2 < planes)
            def _():
                noise_copy(c + 2).start()

        def add(p, j, slot):
            wide = parts[p, :, rows(j)].astype(jnp.float32) + landed[p, slot].astype(jnp.float32)
            parts[p, :, rows(j)] = wide.astype(jnp.bfloat16)

        rising = c - me
        for far in range(count - 1, 0, -1):
            @pl.when(jnp.logical_and(inside(rising), me + far <= count - 1))
            def _():
                j = me + far

                @pl.when(has_down)
                def _():
                    sum_copy(rising, j, 0, j).wait_recv()
                    add(rising, j, j)

                sum_copy(rising, j, 0, j).start()

        sinking = c - (count - 1 - me)
        for far in range(count - 1, 0, -1):
            @pl.when(jnp.logical_and(inside(sinking), me - far >= 0))
            def _():
                j = me - far

                @pl.when(has_up)
                def _():
                    sum_copy(sinking, j, 1, j).wait_recv()
                    add(sinking, j, j)

                sum_copy(sinking, j, 1, count if far == 1 else j).start()

        done = c - (count - 1)

        @pl.when(inside(done))
        def _():
            @pl.when(has_down)
            def _():
                sum_copy(done, me, 0, me).wait_recv()
                add(done, me, me)

            @pl.when(has_up)
            def _():
                sum_copy(done, me, 1, count).wait_recv()
                add(done, me, count)

            for part in range(2):
                whole = parts[done, part, rows(me)]
                for h in range(row_count):
                    halves[done, h, part] = whole[:, h * row_block : (h + 1) * row_block]
            for at in range(len(offsets)):
                last_copy(done, at, False).start()

        return carry

    lax.fori_loop(0, planes + 2 * count - 2, step, 0)

    def finish(p, carry):
        for j in range(count):
            @pl.when(jnp.logical_and(has_up, j <= me))
            def _():
                gather_copy(p, j, 0).wait_send()

            @pl.when(jnp.logical_and(has_down, j >= me))
            def _():
                gather_copy(p, j, 1).wait_send()

            @pl.when(j > me)
            def _():
                sum_copy(p, j, 0, j).wait_send()

            @pl.when(j < me)
            def _():
                sum_copy(p, j, 1, j).wait_send()

        for dh in range(1, row_count):
            half_copy(p, dh, row).wait_send()
        last_copy(p, 0, False).wait()
        for at in range(1, len(offsets)):
            last_copy(p, at, False).wait_send()
            last_copy(p, at, True).wait_recv()
        return carry

    lax.fori_loop(0, planes, finish, 0)


def slab_planes(own_modes, noise_field, mode_table, turned):
    count = lax.axis_size("my")
    mode_count = mode_table.shape[0]
    row_count = lax.axis_size("mx")
    rep_count = lax.axis_size("rep")
    planes_rep, _, block, row_block = own_modes.shape
    planes = planes_rep // row_count
    point_block, point_count = noise_field.shape[2:]
    vmem = pl.BlockSpec(memory_space=pltpu.VMEM)
    hbm = pl.BlockSpec(memory_space=pl.ANY)
    dma = pltpu.SemaphoreType.DMA
    flops = 8 * planes * mode_count * point_block * (point_count + mode_count)
    return pl.pallas_call(
        slab_kernel,
        out_shape=jax.ShapeDtypeStruct((planes_rep * rep_count, 2, block, row_block), jnp.bfloat16),
        in_specs=[hbm, hbm, vmem, vmem],
        out_specs=hbm,
        scratch_shapes=[
            pltpu.VMEM((planes, 2, mode_count, mode_count), jnp.bfloat16),
            pltpu.VMEM((planes, 2, mode_count, mode_count), jnp.bfloat16),
            pltpu.VMEM((planes, count + 1, 2, block, mode_count), jnp.bfloat16),
            pltpu.VMEM((2, 2, point_block, point_count), jnp.bfloat16),
            pltpu.VMEM((planes, row_count, 2, block, row_block), jnp.bfloat16),
            dma,
            dma((2,)),
            dma((planes, count)),
            dma((planes, 2, count)),
            dma((planes, count + 1)),
            dma((planes, 2, count)),
            dma((planes, row_count)),
            dma((planes, row_count)),
            dma((planes, row_count * rep_count)),
            dma((planes, row_count * rep_count)),
        ],
        compiler_params=pltpu.CompilerParams(
            collective_id=0, has_side_effects=True, vmem_limit_bytes=60 * 1024 * 1024
        ),
        cost_estimate=pl.CostEstimate(
            flops=flops, bytes_accessed=noise_field.size * 2, transcendentals=0
        ),
    )(own_modes, noise_field, mode_table, turned)


def body(coefficients, noise_field, mode_table):
    rep_index = lax.axis_index("rep")
    col_index = lax.axis_index("my")
    rep_count = lax.axis_size("rep")
    row_count = lax.axis_size("mx")
    col_count = lax.axis_size("my")
    planes_dev = noise_field.shape[0]
    planes_rep = planes_dev * row_count
    planes_all = planes_rep * rep_count
    mode_count = mode_table.shape[0]
    point_count = mode_table.shape[1]
    slab_first = point_count // 2 - planes_all // 2
    row_block = mode_count // row_count
    col_block = mode_count // col_count
    point_block = point_count // col_count
    own_block = mode_count // rep_count
    if col_block % 16 or point_block % 128 or mode_count % 128 or col_count < 2:
        return plain_body(coefficients, noise_field, mode_table)
    slab_own = lax.dynamic_slice_in_dim(
        mode_table, slab_first + rep_index * planes_rep, planes_rep, 1
    )
    zmodes = jnp.einsum(
        "pabk,kz->zpba", coefficients, slab_own, preferred_element_type=jnp.float32
    ).astype(jnp.bfloat16)
    turned = lax.dynamic_slice_in_dim(mode_table, col_index * point_block, point_block, 1).T
    plane_grid = slab_planes(zmodes, noise_field, mode_table, turned)
    slab_back = lax.dynamic_slice_in_dim(mode_table, rep_index * own_block, own_block, 0)[
        :, slab_first : slab_first + planes_all
    ]
    summed = jnp.einsum("zpba,nz->pabn", plane_grid, slab_back, preferred_element_type=jnp.float32)
    return summed.astype(jnp.bfloat16)


def solution(mesh):
    in_specs = (P(None, "mx", "my", None), P(("rep", "mx"), None, "my", None), P())
    out_specs = P(None, "mx", "my", "rep")
    return jax.shard_map(body, mesh=mesh, in_specs=in_specs, out_specs=out_specs, check_vma=False)
```
